256 devices in a mesh: row: 8 (over x_hi, y), col: 32 (over x_lo, z, core).
Axes of the slice: x: 4 (x_hi: 2, x_lo: 2; x = x_hi * 2 + x_lo), y: 4, z: 8, core: 2. Of those that a mesh axis runs over, the one named last changes fastest.
Arguments:
- out_grad: bfloat16 [32768, 512], P('col', 'row'), may hold values from -6 to 6
- node_in: bfloat16 [32768, 512], P(('row', 'col')), may hold values from -0.03125 to 0.03125
- weights: bfloat16 [3, 512, 512], replicated, may hold values from -0.25 to 0.25
- tile_vals: bfloat16 [3, 32, 8, 32, 128, 128], P(None, 'col', 'row'), may hold values from -0.15625 to 0.15625
- tile_rows: int32 [3, 32, 8, 32], P(None, 'col', 'row'), may hold values from 0 to 7
- tile_cols: int32 [3, 32, 8, 32], P(None, 'col', 'row'), may hold values from 0 to 31
- tile_count: int32 [3, 32, 8], P(None, 'col', 'row'), may hold values from 1 to 32, as said below
Outputs:
- d_nodes: bfloat16 [32768, 512], P(('row', 'col'))
- d_weights: float32 [3, 512, 512], replicated
The draws below stay inside these ranges and needn't reach their ends.
Inputs may be any that keep to these rules, and one draw needn't show every extreme that they name: Only the first tile_count slots of a block's list hold tiles; later slots are ignored. In every relation some block uses all 32 slots. `tile_rows`: coordinates may repeat within a block's list; such tiles add.
All inputs are finite; a program needn't handle non-finite values.
Results may differ from the reference program's by a relative error of at most 0.005.
Values may be sent and summed in bfloat16 or wider, within the bound.
A program may use at most 256 MiB of HBM per device.

```python
import jax
import jax.numpy as jnp
from jax import lax

D = 512
R = 3
TILE = 128
N_DEV = 128
CAP = 32
ROW_GROUPS = 8
COL_GROUPS = 32
NODES = 32768
TR = 8
TC = 32


def draw_tile_count(key, part):
    grid_shape = (R, COL_GROUPS, ROW_GROUPS)
    levels = jax.random.randint(jax.random.fold_in(key, 11), grid_shape, 1, 9)
    counts = jnp.maximum(1, CAP * levels * levels // 64)
    full_device = jax.random.randint(jax.random.fold_in(key, 12), (R,), 0, COL_GROUPS * ROW_GROUPS)
    flat_counts = counts.reshape(R, COL_GROUPS * ROW_GROUPS)
    chosen = jnp.arange(COL_GROUPS * ROW_GROUPS)[None, :] == full_device[:, None]
    flat_counts = jnp.where(chosen, CAP, flat_counts)
    return flat_counts.reshape(grid_shape).astype(jnp.int32)


def touch_ends(array, own_key, least, largest):
    extent = array.shape
    place = [jax.random.randint(jax.random.fold_in(own_key, axis), (), 0, extent[axis]) for axis in range(len(extent))]
    array = array.at[tuple(place)].set(least)
    longest = extent.index(max(extent))
    place[longest] = (place[longest] + 1) % extent[longest]
    return array.at[tuple(place)].set(largest)


def shard_levels(rng, shape, cuts, low, largest):
    def one(position, blocks):
        draws = jax.random.uniform(jax.random.fold_in(jax.random.fold_in(rng, 6), position), (blocks,), jnp.float32, low / len(cuts), largest / len(cuts))
        return jnp.repeat(jnp.exp(draws), shape[position] // blocks).reshape((-1,) + (1,) * (len(shape) - position - 1))

    loudness = one(*cuts[0])
    for cut in cuts[1:]:
        loudness = loudness * one(*cut)
    return loudness


def bell_draw(stream_key, dims, spread, most, split=(), held_as=jnp.bfloat16):
    drawn = spread * jax.random.normal(stream_key, dims, jnp.float32)
    if split:
        drawn = drawn * shard_levels(stream_key, dims, split, -0.22, 0.18)
    return jnp.clip(drawn, -most, most).astype(held_as)


def setup_inputs(seed: int = 0) -> dict:
    streams_of = jax.random.split(jax.random.key(seed), 8)
    out_grad = bell_draw(streams_of[0], (NODES, D), 1.0, 6.0, ((0, 32), (1, 8)))
    node_in = bell_draw(streams_of[1], (NODES, D), NODES ** -0.5, 0.03125, ((0, 256),))
    weights = bell_draw(streams_of[2], (R, D, D), D ** -0.5, 0.25)
    tile_vals = bell_draw(streams_of[3], (R, COL_GROUPS, ROW_GROUPS, CAP, TILE, TILE), (CAP * COL_GROUPS * 2 * TILE // (5 * TC)) ** -0.5, 0.15625, ((1, 32), (2, 8)))
    tile_rows = touch_ends(jax.random.randint(streams_of[4], (R, COL_GROUPS, ROW_GROUPS, CAP), 0, TR), jax.random.fold_in(streams_of[4], 1), 0, TR - 1).astype(jnp.int32)
    tile_cols = touch_ends(jax.random.randint(streams_of[5], (R, COL_GROUPS, ROW_GROUPS, CAP), 0, TC), jax.random.fold_in(streams_of[5], 1), 0, TC - 1).astype(jnp.int32)
    tile_count = draw_tile_count(jax.random.fold_in(streams_of[7], 71), 0)
    return {"out_grad": out_grad, "node_in": node_in, "weights": weights, "tile_vals": tile_vals, "tile_rows": tile_rows, "tile_cols": tile_cols, "tile_count": tile_count}


def block_products(operand, tile_block, row_ids, col_ids, count_now, block_index):
    group_col = block_index // ROW_GROUPS
    group_row = block_index % ROW_GROUPS
    lanes = jnp.arange(TILE, dtype=jnp.int32)
    source_ids = (group_col * (N_DEV * ROW_GROUPS) + row_ids[:, None] * TILE + lanes[None, :]).astype(jnp.int32)
    sources = jnp.take(operand, source_ids.reshape(-1), axis=0).reshape(CAP, TILE, 2 * D)
    live = (jnp.arange(CAP, dtype=jnp.int32) < count_now).astype(jnp.float32)
    products = jnp.einsum("skt,skd->std", tile_block.astype(jnp.float32), sources.astype(jnp.float32), precision=lax.Precision.HIGHEST)
    products = products * live[:, None, None]
    target_ids = (group_row * (N_DEV * COL_GROUPS) + col_ids[:, None] * TILE + lanes[None, :]).astype(jnp.int32)
    return target_ids.reshape(-1), products.reshape(CAP * TILE, 2 * D)


def reference(out_grad, node_in, weights, tile_vals, tile_rows, tile_cols, tile_count):
    blocks = COL_GROUPS * ROW_GROUPS
    block_ids = jnp.arange(blocks, dtype=jnp.int32)
    mixed_total = jnp.zeros((NODES, D), jnp.float32)
    weight_grads = []
    inputs_wide = node_in.astype(jnp.float32)
    for relation in range(R):
        premixed = jnp.dot(out_grad, weights[relation].T, preferred_element_type=jnp.float32).astype(jnp.bfloat16)
        operand = jnp.concatenate([out_grad, premixed], axis=1)

        def block_step(summed, inputs):
            target_ids, products = block_products(operand, inputs[0], inputs[1], inputs[2], inputs[3], inputs[4])
            return summed.at[target_ids].add(products), None

        scanned = (tile_vals[relation].reshape(blocks, CAP, TILE, TILE), tile_rows[relation].reshape(blocks, CAP), tile_cols[relation].reshape(blocks, CAP), tile_count[relation].reshape(blocks), block_ids)
        start_sums = jnp.zeros((NODES, 2 * D), jnp.float32)
        summed, ignored = lax.scan(block_step, start_sums, scanned)
        weight_grads.append(jnp.dot(inputs_wide.T, summed[:, :D], precision=lax.Precision.HIGHEST))
        mixed_total = mixed_total + summed[:, D:]
    return mixed_total.astype(jnp.bfloat16), jnp.stack(weight_grads)
```

```python
import functools

import jax
import jax.numpy as jnp
from jax import lax
from jax.experimental import pallas as pl
from jax.experimental.pallas import tpu as pltpu
from jax.sharding import Mesh
from jax.sharding import PartitionSpec as P

AXES = ("xh", "y", "xl", "z", "core")
ROW = ("xh", "y")
COL = ("xl", "z", "core")

TILE = 128
SLOTS = 96
UNROLL = 4
M_SLOT, M_ROW, M_KEEP, M_END, H_SLOT, H_COL, H_KEEP, H_END = range(8)
F32 = jnp.float32
BF16 = jnp.bfloat16


def index_table(tile_rows, tile_cols, tile_count):
    relations, cap = tile_rows.shape
    i = jnp.arange(relations * cap, dtype=jnp.int32)
    relation = i // cap
    live = (jnp.arange(cap, dtype=jnp.int32)[None, :] < tile_count[:, None]).reshape(-1)
    row = tile_rows.reshape(-1)
    col = tile_cols.reshape(-1)

    def ordered(key, other):
        unique = key * 128 + i
        rank = jnp.sum((unique[None, :] < unique[:, None]).astype(jnp.int32), axis=1)
        hot = (rank[None, :] == i[:, None]).astype(jnp.int32)
        take = lambda v: jnp.sum(hot * v[None, :], axis=1)
        sorted_key = take(key)
        before = jnp.concatenate([jnp.full((1,), -1, jnp.int32), sorted_key[:-1]])
        return take(i), take(other), (sorted_key == before).astype(jnp.int32), rank

    def ends(key, rank, count):
        j = jnp.arange(count, dtype=jnp.int32)
        mine = (key[None, :] == j[:, None]) & live[None, :]
        return jnp.max(jnp.where(mine, rank[None, :], -1), axis=1)

    key_m = jnp.where(live, col, 64)
    slot_m, row_m, keep_m, rank_m = ordered(key_m, relation * 8 + row)
    key_h = relation * 16 + jnp.where(live, row, 15)
    slot_h, col_h, keep_h, rank_h = ordered(key_h, col)
    end_m = ends(col, rank_m, 32)
    end_h = ends(relation * 8 + row, rank_h, 24)
    pad = lambda v: jnp.pad(v, (0, 128 - v.shape[0]))
    return jnp.stack(
        [pad(v) for v in (slot_m, row_m, keep_m, end_m, slot_h, col_h, keep_h, end_h)]
    )


def kernel(
    idx, og, nin, w_hbm, t_hbm, dn_out, dw_out,
    gp, g, nb, w, tiles, pre, acc, cum, hs,
    sc, rc, s, rx, rz, rxb, ds_, dr, da, dy, ry, dxf, dxs, rxd, dz, rzd, dzg,
    send_sem, recv_sem, local_sem,
):
    xh, y, xl, z, core = (lax.axis_index(a) for a in AXES)
    ny, nz = lax.axis_size("y"), lax.axis_size("z")
    q = xh * ny + y
    xi = xh * 2 + xl
    other_xl, other_core, other_xh = 1 - xl, 1 - core, 1 - xh
    mod = lambda v, n: lax.rem(v + 2 * n, n)
    zz = lambda d: mod(z + d, nz)
    yy = lambda d: mod(y + d, ny)

    def peer(**kw):
        base = {"xh": xh, "y": y, "xl": xl, "z": z, "core": core}
        base.update(kw)
        return tuple(base[a] for a in AXES)

    def xpeer(d):
        there = mod(xi + d, 4)
        return there, peer(xh=there // 2, xl=there % 2)

    to_z = {1: peer(z=zz(1)), -1: peer(z=zz(-1))}
    to_y = {1: peer(y=yy(1)), -1: peer(y=yy(-1))}
    to_x = peer(xl=other_xl)
    to_core = peer(core=other_core)
    to_xh = peer(xh=other_xh)

    copies = []

    def send(src, dst, device):
        m = len(copies)
        copy = pltpu.make_async_remote_copy(
            src_ref=src, dst_ref=dst, send_sem=send_sem.at[m], recv_sem=recv_sem.at[m],
            device_id=device, device_id_type=pl.DeviceIdType.MESH,
        )
        copy.start()
        copies.append(copy)
        return copy

    barrier = pltpu.get_barrier_semaphore()
    others = [peer(z=zz(d)) for d in range(1, 8)] + [xpeer(d)[1] for d in (1, 2, 3)]
    others += [to_y[1], to_y[-1], to_core]
    for device in others:
        pl.semaphore_signal(barrier, inc=1, device_id=device, device_id_type=pl.DeviceIdType.MESH)
    load_w = pltpu.make_async_copy(w_hbm, w, local_sem.at[0])
    load_w.start()
    load_t = pltpu.make_async_copy(t_hbm, tiles, local_sem.at[1])
    load_t.start()
    gp[q] = jnp.concatenate([og[:512], og[512:]], axis=1)
    slot = lambda a, b, c: (a * nz + b) * 2 + c
    own = slot(xl, z, core)
    nb[own] = nin[...]
    pl.semaphore_wait(barrier, len(others))

    g_xh = send(gp.at[q], gp.at[q], to_xh)
    g_y = {d: send(gp.at[q], gp.at[q], to_y[d]) for d in (1, -1)}
    half = {1: pl.ds(0, 256), -1: pl.ds(256, 256)}
    T, B, XLO, XHI = pl.ds(0, 64), pl.ds(64, 64), pl.ds(64, 32), pl.ds(96, 32)

    def nsend(a, b, rows, device, c=core):
        ref = nb.at[slot(a, b, c), rows]
        return send(ref, ref, device)

    n_bx = send(nin.at[B], nb.at[own, B], to_x)
    n_z = {}
    for d in (1, -1):
        n_z[d, 0, "T"] = send(nin.at[T], nb.at[own, T], to_z[d])
        n_z[d, 0, "B"] = send(nin.at[B], nb.at[own, B], to_z[d])
    n_tx = {0: send(nin.at[T], nb.at[own, T], to_x)}
    n_core = [send(nin, nb.at[own], to_core)]

    def g_forward(copies_in, column):
        out = []
        for d in (1, -1):
            copies_in[d].wait_recv()
            ref = gp.at[column * ny + yy(-d), half[d]]
            out.append(send(ref, ref, to_y[d]))
        return out

    def n_step(k):
        for d in (1, -1):
            origin = zz(-d * k)
            pieces = {"T": T, "B": B, "X": B}
            if k == 4:
                pieces = {"T": T, "X": XLO} if d == 1 else {"B": B, "X": XHI}
            onward = pieces if k < 3 else ({"T": T, "X": XLO} if d == 1 else {"B": B, "X": XHI})
            for name, rows in pieces.items():
                n_z[d, k - 1, name].wait_recv()
                if k < 4 and name in onward:
                    column = other_xl if name == "X" else xl
                    n_z[d, k, name] = nsend(column, origin, onward[name], to_z[d])
                if name == "T":
                    n_tx[-d * k] = nsend(xl, origin, T, to_x)
            if k < 4:
                n_core.append(nsend(xl, origin, pl.ds(0, 128), to_core))
                n_core.append(nsend(other_xl, origin, B, to_core))
        if k == 4:
            n_core.append(nsend(xl, zz(4), pl.ds(0, 128), to_core))
            n_core.append(nsend(other_xl, zz(4), B, to_core))

    def n_top(d):
        n_tx[d].wait_recv()
        n_core.append(nsend(other_xl, zz(d), T, to_core))

    g_half = g_forward(g_y, xh)
    n_bx.wait_recv()
    for d in (1, -1):
        n_z[d, 0, "X"] = nsend(other_xl, z, B, to_z[d])
    n_core.append(nsend(other_xl, z, B, to_core))
    g_xh.wait_recv()
    other_q = other_xh * ny + y
    g_y2 = {d: send(gp.at[other_q], gp.at[other_q], to_y[d]) for d in (1, -1)}
    n_step(1)
    g_half2 = g_forward(g_y2, other_xh)
    n_step(2)
    for copy in g_half + g_half2:
        copy.wait_recv()

    first = lax.broadcasted_iota(jnp.int32, (512, 128), 1) < 64
    for k in range(4):
        a = gp[2 * k].astype(F32)
        b = gp[2 * k + 1].astype(F32)
        lanes = pl.ds(k * 128, 128)
        g[:512, lanes] = jnp.where(first, a, pltpu.roll(b, 64, 1)).astype(BF16)
        g[512:, lanes] = jnp.where(first, pltpu.roll(a, 64, 1), b).astype(BF16)
    load_w.wait()
    n_step(3)

    def premix(i, carry):
        r, block = i // 4, i % 4
        rows = pl.ds(pl.multiple_of(block * 256, 256), 256)
        mixed = lax.dot_general(
            g[rows, :], w[r], (((1,), (1,)), ((), ())), preferred_element_type=F32
        )
        at = r * 8 + block * 2
        pre[pl.ds(at, 2)] = mixed.astype(BF16).reshape(2, 128, 512)
        return carry

    lax.fori_loop(0, 12, premix, 0)
    load_t.wait()

    def products(first_slot, count, slot_row, other_row, keep_row, operand, contract):
        def step(i, carry):
            for u in range(UNROLL):
                k = first_slot + i * UNROLL + u
                tile = tiles[idx[slot_row, k]]
                other = operand[idx[other_row, k]]
                product = lax.dot_general(
                    tile, other, (((contract,), (0,)), ((), ())), preferred_element_type=F32
                )
                total = jnp.where(idx[keep_row, k] > 0, acc[...], 0.0) + product
                acc[...] = total
                cum[k] = total.astype(BF16)
            return carry

        lax.fori_loop(0, count // UNROLL, step, 0)

    acc[...] = jnp.zeros_like(acc)
    products(0, 48, M_SLOT, M_ROW, M_KEEP, pre, 0)
    n_step(4)
    for d in (0, 1, -1):
        n_top(d)
    products(48, 48, M_SLOT, M_ROW, M_KEEP, pre, 0)
    for d in (2, -2, 3, -3, -4):
        n_top(d)

    def own_sum(j):
        end = idx[M_END, j]
        value = cum[jnp.maximum(end, 0)]
        return jnp.where(end >= 0, value.astype(F32), 0.0)

    order = (4, 3, -3, 2, -2, 1, -1, 0)
    s_core, s_x, s_z = {}, {}, {}
    for d in order:
        at = zz(d)
        for a in range(2):
            sc[at, a] = own_sum(slot(a, at, other_core)).astype(BF16)
        s_core[d] = send(sc.at[at], rc.at[at], to_core)
    for d in order:
        at = zz(d)
        s_core[d].wait_recv()
        for a in range(2):
            total = own_sum(slot(a, at, core)) + rc[at, a].astype(F32)
            s[at, a] = total.astype(BF16)
        s_x[d] = send(s.at[at, other_xl, T], rx.at[at], to_x)

    LO, HI, ALL = pl.ds(0, 32), pl.ds(32, 32), pl.ds(0, 64)
    piece_of = {"T": 0, "B": 1, "X": 2}

    def s_send(d, step, name, rows_src, rows_dst):
        at = zz(d * (4 - step))
        column = other_xl if name == "X" else xl
        p = 0 if d == 1 else 1
        s_z[d, step, name] = send(
            s.at[at, column, rows_src], rz.at[p, step, piece_of[name], rows_dst], to_z[d]
        )

    def add_rows(at, column, rows, *terms):
        total = s[at, column, rows].astype(F32)
        for term in terms:
            total = total + term.astype(F32)
        s[at, column, rows] = total.astype(BF16)

    def s_step(step):
        if step == 0:
            s_x[4].wait_recv()
            add_rows(zz(4), xl, T, rx[zz(4)])
            s_send(1, 0, "T", T, ALL)
            s_send(-1, 0, "B", B, ALL)
            s_send(1, 0, "X", XLO, LO)
            s_send(-1, 0, "X", XHI, HI)
            return
        for d in (1, -1):
            far = d * (4 - step)
            at = zz(far)
            p = 0 if d == 1 else 1
            s_x[far].wait_recv()
            tops = [rx[at]]
            if step > 1 or d == 1:
                s_z[d, step - 1, "T"].wait_recv()
                tops.append(rz[p, step - 1, 0])
            add_rows(at, xl, T, *tops)
            s_send(d, step, "T", T, ALL)
            if step > 1 or d == -1:
                s_z[d, step - 1, "B"].wait_recv()
                add_rows(at, xl, B, rz[p, step - 1, 1])
            s_send(d, step, "B", B, ALL)
            s_z[d, step - 1, "X"].wait_recv()
            if step > 1:
                add_rows(at, other_xl, B, rz[p, step - 1, 2])
            elif d == 1:
                add_rows(at, other_xl, XLO, rz[p, 0, 2, LO])
            else:
                add_rows(at, other_xl, XHI, rz[p, 0, 2, HI])
            s_send(d, step, "X", B, ALL)

    def s_last():
        for d in (1, -1):
            s_z[d, 3, "X"].wait_recv()
        add_rows(z, other_xl, B, rz[0, 3, 2], rz[1, 3, 2])
        final = send(s.at[z, other_xl, B], rxb, to_x)
        s_x[0].wait_recv()
        for d in (1, -1):
            s_z[d, 3, "T"].wait_recv()
        top = s[z, xl, T].astype(F32) + rx[z].astype(F32)
        top = top + rz[0, 3, 0].astype(F32) + rz[1, 3, 0].astype(F32)
        dn_out[T] = top.astype(BF16)
        for d in (1, -1):
            s_z[d, 3, "B"].wait_recv()
        bottom = s[z, xl, B].astype(F32) + rz[0, 3, 1].astype(F32) + rz[1, 3, 1].astype(F32)
        final.wait_recv()
        dn_out[B] = (bottom + rxb[...].astype(F32)).astype(BF16)

    d_copy = {}
    own_rows = lambda start, n: pl.ds(pl.multiple_of(start, n), n)

    def weight_grad(r):
        products(r * 32, 32, H_SLOT, H_COL, H_KEEP, nb, 1)
        for i in range(8):
            end = idx[H_END, r * 8 + i]
            value = cum[jnp.maximum(end, 0)]
            hs[pl.ds(i * 128, 128)] = jnp.where(end >= 0, value.astype(F32), 0.0).astype(BF16)

        def block(which, to):
            lanes = pl.ds(pl.multiple_of(which * 256, 256), 256)
            part = lax.dot_general(
                hs[:, lanes], g[...], (((0,), (0,)), ((), ())), preferred_element_type=F32
            )
            to[r] = part.astype(to.dtype)

        block(other_core, ds_)
        d_copy["core", r] = send(ds_.at[r], dr.at[r], to_core)
        block(core, da)

    yrow = lambda v: own_rows(v * 64, 64)
    yhalf = {1: lambda v: own_rows(v * 64, 32), -1: lambda v: own_rows(v * 64 + 32, 32)}

    def stage_y0(r):
        d_copy["core", r].wait_recv()
        da[r] = da[r] + dr[r].astype(F32)
        far = yy(2)
        dy[r, yrow(far)] = da[r, yrow(far)].astype(BF16)
        for d in (1, -1):
            d_copy["y0", d, r] = send(dy.at[r, yhalf[d](far)], ry.at[r, 0, half32[d]], to_y[d])

    half32 = {1: pl.ds(0, 32), -1: pl.ds(32, 32)}

    def stage_y1(r):
        for d in (1, -1):
            there = yy(d)
            d_copy["y0", d, r].wait_recv()
            rows = yhalf[d](there)
            da[r, rows] = da[r, rows] + ry[r, 0, half32[d]].astype(F32)
            dy[r, yrow(there)] = da[r, yrow(there)].astype(BF16)
            p = 1 if d == 1 else 2
            d_copy["y1", d, r] = send(dy.at[r, yrow(there)], ry.at[r, p], to_y[d])

    def stage_x(r):
        for d in (1, -1):
            d_copy["y1", d, r].wait_recv()
        total = da[r, yrow(y)] + ry[r, 1].astype(F32) + ry[r, 2].astype(F32)
        dxf[r] = total
        dxs[r] = total.astype(BF16)
        for d in (1, 2, 3):
            there, device = xpeer(d)
            d_copy["x", d, r] = send(dxs.at[r, own_rows(there * 16, 16)], rxd.at[r, d - 1], device)

    def zpart(v):
        return own_rows(lax.rem(v, 2) * 8, 8), pl.ds(pl.multiple_of((v // 2) * 128, 128), 128)

    def stage_z(r):
        for d in (1, 2, 3):
            d_copy["x", d, r].wait_recv()
        total = dxf[r, own_rows(xi * 16, 16)]
        for d in (1, 2, 3):
            total = total + rxd[r, d - 1].astype(F32)
        dz[r] = total
        for d in range(1, 8):
            rows, lanes = zpart(zz(d))
            d_copy["z", d, r] = send(dz.at[r, rows, lanes], rzd.at[r, d - 1], peer(z=zz(d)))

    def stage_zg(r):
        rows, lanes = zpart(z)
        total = dz[r, rows, lanes]
        for d in range(1, 8):
            d_copy["z", d, r].wait_recv()
            total = total + rzd[r, d - 1]
        dzg[r, rows, lanes] = total
        ref = dzg.at[r, rows, lanes]
        for d in range(1, 8):
            d_copy["zg", d, r] = send(ref, ref, peer(z=zz(d)))

    def out_rows(c, yv, n, offset=0):
        return own_rows(c * 256 + yv * 64 + offset, n)

    def stage_xg(r):
        for d in range(1, 8):
            d_copy["zg", d, r].wait_recv()
        rows = own_rows(core * 256 + y * 64 + xi * 16, 16)
        dw_out[r, rows] = dzg[r].astype(BF16)
        ref = dw_out.at[r, rows]
        for d in (1, 2, 3):
            d_copy["xg", d, r] = send(ref, ref, xpeer(d)[1])

    def stage_yg0(r):
        for d in (1, 2, 3):
            d_copy["xg", d, r].wait_recv()
        ref = dw_out.at[r, out_rows(core, y, 64)]
        for d in (1, -1):
            d_copy["yg0", d, r] = send(ref, ref, to_y[d])
        d_copy["cg0", r] = send(ref, ref, to_core)

    def stage_yg1(r):
        for d in (1, -1):
            d_copy["yg0", d, r].wait_recv()
            came = yy(-d)
            ref = dw_out.at[r, out_rows(core, came, 32, 0 if d == 1 else 32)]
            d_copy["yg1", d, r] = send(ref, ref, to_y[d])
            ref = dw_out.at[r, out_rows(core, came, 64)]
            d_copy["cg1", d, r] = send(ref, ref, to_core)

    def stage_cg(r):
        for d in (1, -1):
            d_copy["yg1", d, r].wait_recv()
        ref = dw_out.at[r, out_rows(core, yy(2), 64)]
        d_copy["cg2", r] = send(ref, ref, to_core)

    def stage_end(r):
        d_copy["cg0", r].wait_recv()
        for d in (1, -1):
            d_copy["cg1", d, r].wait_recv()
        d_copy["cg2", r].wait_recv()

    for copy in n_core:
        copy.wait_recv()
    s_step(0)
    weight_grad(0)
    s_step(1)
    weight_grad(1)
    stage_y0(0)
    s_step(2)
    weight_grad(2)
    stage_y0(1)
    stage_y1(0)
    stage_y0(2)
    s_step(3)
    stage_y1(1)
    stage_x(0)
    stage_y1(2)
    stage_x(1)
    stage_z(0)
    stage_x(2)
    stage_z(1)
    stage_zg(0)
    stage_z(2)
    stage_zg(1)
    stage_xg(0)
    stage_zg(2)
    stage_xg(1)
    stage_yg0(0)
    stage_xg(2)
    s_last()
    stage_yg0(1)
    stage_yg1(0)
    stage_yg0(2)
    stage_yg1(1)
    stage_cg(0)
    stage_yg1(2)
    stage_cg(1)
    stage_cg(2)
    for r in range(3):
        stage_end(r)
    for copy in copies:
        copy.wait_send()


MESSAGES = 232


def run(idx, out_grad, node_in, weights, tiles):
    vmem = pl.BlockSpec(memory_space=pltpu.VMEM)
    hbm = pl.BlockSpec(memory_space=pl.ANY)
    scratch = [
        pltpu.VMEM((8, 512, 128), BF16),
        pltpu.VMEM((1024, 512), BF16),
        pltpu.VMEM((32, 128, 512), BF16),
        pltpu.VMEM((3, 512, 512), BF16),
        pltpu.VMEM((SLOTS, TILE, TILE), BF16),
        pltpu.VMEM((24, 128, 512), BF16),
        pltpu.VMEM((128, 512), F32),
        pltpu.VMEM((SLOTS, 128, 512), BF16),
        pltpu.VMEM((1024, 512), BF16),
        pltpu.VMEM((8, 2, 128, 512), BF16),
        pltpu.VMEM((8, 2, 128, 512), BF16),
        pltpu.VMEM((8, 2, 128, 512), BF16),
        pltpu.VMEM((8, 64, 512), BF16),
        pltpu.VMEM((2, 4, 3, 64, 512), BF16),
        pltpu.VMEM((64, 512), BF16),
        pltpu.VMEM((3, 256, 512), BF16),
        pltpu.VMEM((3, 256, 512), BF16),
        pltpu.VMEM((3, 256, 512), F32),
        pltpu.VMEM((3, 256, 512), BF16),
        pltpu.VMEM((3, 3, 64, 512), BF16),
        pltpu.VMEM((3, 64, 512), F32),
        pltpu.VMEM((3, 64, 512), BF16),
        pltpu.VMEM((3, 3, 16, 512), BF16),
        pltpu.VMEM((3, 16, 512), F32),
        pltpu.VMEM((3, 7, 8, 128), F32),
        pltpu.VMEM((3, 16, 512), F32),
        pltpu.SemaphoreType.DMA((MESSAGES,)),
        pltpu.SemaphoreType.DMA((MESSAGES,)),
        pltpu.SemaphoreType.DMA((2,)),
    ]
    return pl.pallas_call(
        kernel,
        out_shape=(
            jax.ShapeDtypeStruct((128, 512), BF16),
            jax.ShapeDtypeStruct((3, 512, 512), BF16),
        ),
        in_specs=[pl.BlockSpec(memory_space=pltpu.SMEM), vmem, vmem, hbm, hbm],
        out_specs=(vmem, vmem),
        scratch_shapes=scratch,
        compiler_params=pltpu.CompilerParams(
            collective_id=0, has_side_effects=True, vmem_limit_bytes=62 * 2**20
        ),
        name="fused",
    )(idx, out_grad, node_in, weights, tiles)


def body(out_grad, node_in, weights, tile_vals, tile_rows, tile_cols, tile_count):
    idx = index_table(tile_rows[:, 0, 0], tile_cols[:, 0, 0], tile_count[:, 0, 0])
    tiles = tile_vals.reshape(SLOTS, TILE, TILE)
    d_nodes, d_weights = run(idx, out_grad, node_in, weights, tiles)
    return d_nodes, d_weights.astype(F32)


def solution(mesh):
    finer = Mesh(mesh.devices.reshape(2, 4, 2, 8, 2), AXES)
    in_specs = (
        P(COL, ROW),
        P(ROW + COL, None),
        P(),
        P(None, COL, ROW, None, None, None),
        P(None, COL, ROW, None),
        P(None, COL, ROW, None),
        P(None, COL, ROW),
    )
    out_specs = (P(ROW + COL, None), P())
    return jax.shard_map(body, mesh=finer, in_specs=in_specs, out_specs=out_specs, check_vma=False)
```
